16 devices in a mesh: dp: 4 (over z, y), tp: 4 (over x, core).
Axes of the slice: x: 2, y: 2, z: 2, core: 2. Of those that a mesh axis runs over, the one named last changes fastest.
Arguments:
- hidden_in: bfloat16 [8, 2048, 1280], P('dp', 'tp'), parts along dimension 0
- norms: float32 [2, 4, 1280], replicated
- w_qkv: bfloat16 [2, 1280, 3, 20, 64], P(None, None, None, 'tp')
- w_out: bfloat16 [2, 20, 64, 1280], P(None, 'tp')
- b_out: float32 [2, 1280], replicated
- w_up: bfloat16 [2, 1280, 5120], P(None, None, 'tp')
- b_up: float32 [2, 5120], P(None, 'tp')
- w_down: bfloat16 [2, 5120, 1280], P(None, 'tp')
- b_down: float32 [2, 1280], replicated
Outputs:
- output: bfloat16 [8, 2048, 1280], P('dp', 'tp'), parts along dimension 0
There are 4 independent parts. The reference program is written for one: setup_inputs(seed, part) draws one part's arguments, and reference() takes and returns one part's arrays. A program takes and returns all parts, laid end to end along the dimension named above; an argument that names none is the same for every part.
All inputs are finite; a program needn't handle non-finite values.
Results may differ from the reference program's by a relative error of at most 0.0124455.
Values are sent between devices in bfloat16 or wider.
A program may use at most 1 GiB of HBM per device.

```python
import math
import jax
import jax.numpy as jnp
from jax import lax

N_BATCH = 2
SEQ_LEN = 2048
N_HEADS = 20
HEAD_DIM = 64
FF_DIM = 5120
N_LAYERS = 2

MODEL_DIM = N_HEADS * HEAD_DIM
LN_EPS = 1e-5


def setup_inputs(seed: int = 0, part: int = 0) -> dict:
    base_key = jax.random.key(seed)
    keys = jax.random.split(base_key, 9)
    part_key = jax.random.fold_in(keys[0], part)
    tok_key, scale_key = jax.random.split(part_key)
    tok_scale = jnp.exp(0.4 * jax.random.normal(scale_key, (N_BATCH, SEQ_LEN, 1), jnp.float32))
    hidden_in = (jax.random.normal(tok_key, (N_BATCH, SEQ_LEN, MODEL_DIM), jnp.float32) * tok_scale).astype(jnp.bfloat16)
    norm_base = jnp.array([1.0, 0.0, 1.0, 0.0], jnp.float32)[None, :, None]
    norms = norm_base + 0.2 * jax.random.normal(keys[1], (N_LAYERS, 4, MODEL_DIM), jnp.float32)
    qk_gain = (math.log(SEQ_LEN) / 2.0) ** 0.25
    slot_gain = jnp.array([qk_gain, qk_gain, 1.0], jnp.float32)[None, None, :, None, None]
    w_qkv = (jax.random.normal(keys[2], (N_LAYERS, MODEL_DIM, 3, N_HEADS, HEAD_DIM), jnp.float32) * slot_gain * MODEL_DIM ** -0.5).astype(jnp.bfloat16)
    out_gain = 0.7 * SEQ_LEN ** 0.25 * MODEL_DIM ** -0.5
    w_out = (jax.random.normal(keys[3], (N_LAYERS, N_HEADS, HEAD_DIM, MODEL_DIM), jnp.float32) * out_gain).astype(jnp.bfloat16)
    b_out = 0.2 * jax.random.normal(keys[4], (N_LAYERS, MODEL_DIM), jnp.float32)
    w_up = (jax.random.normal(keys[5], (N_LAYERS, MODEL_DIM, FF_DIM), jnp.float32) * MODEL_DIM ** -0.5).astype(jnp.bfloat16)
    b_up = 0.3 * jax.random.normal(keys[6], (N_LAYERS, FF_DIM), jnp.float32)
    w_down = (jax.random.normal(keys[7], (N_LAYERS, FF_DIM, MODEL_DIM), jnp.float32) * FF_DIM ** -0.5).astype(jnp.bfloat16)
    b_down = 0.2 * jax.random.normal(keys[8], (N_LAYERS, MODEL_DIM), jnp.float32)
    return {'hidden_in': hidden_in, 'norms': norms, 'w_qkv': w_qkv, 'w_out': w_out, 'b_out': b_out, 'w_up': w_up, 'b_up': b_up, 'w_down': w_down, 'b_down': b_down}


def layer_norm(rows, gain, shift):
    row_mean = jnp.mean(rows, axis=-1, keepdims=True)
    centred = rows - row_mean
    row_var = jnp.mean(centred * centred, axis=-1, keepdims=True)
    return (centred * lax.rsqrt(row_var + LN_EPS) * gain + shift).astype(jnp.bfloat16)


def one_head(head_qkv):
    queries = head_qkv[:, 0].astype(jnp.float32)
    keys_h = head_qkv[:, 1].astype(jnp.float32)
    values_h = head_qkv[:, 2].astype(jnp.float32)
    scores = jnp.einsum('bqe,bke->bqk', queries, keys_h) * HEAD_DIM ** -0.5
    attn_prob = jax.nn.softmax(scores, axis=-1).astype(jnp.bfloat16)
    return jnp.einsum('bqk,bke->bqe', attn_prob.astype(jnp.float32), values_h).astype(jnp.bfloat16)


def one_layer(residual, params):
    norm_l, wqkv_l, wout_l, bout_l, wup_l, bup_l, wdown_l, bdown_l = params
    normed = layer_norm(residual, norm_l[0], norm_l[1])
    qkv_heads = jnp.einsum('bsd,dthe->hbtse', normed.astype(jnp.float32), wqkv_l.astype(jnp.float32)).astype(jnp.bfloat16)
    attn_rows = lax.map(one_head, qkv_heads)
    attn_out = jnp.einsum('hbse,hed->bsd', attn_rows.astype(jnp.float32), wout_l.astype(jnp.float32))
    residual = residual + attn_out + bout_l
    normed2 = layer_norm(residual, norm_l[2], norm_l[3])
    hidden = jnp.einsum('bsd,df->bsf', normed2.astype(jnp.float32), wup_l.astype(jnp.float32)) + bup_l
    gelu_out = jax.nn.gelu(hidden, approximate=True).astype(jnp.bfloat16)
    mlp_out = jnp.einsum('bsf,fd->bsd', gelu_out.astype(jnp.float32), wdown_l.astype(jnp.float32))
    residual = residual + mlp_out + bdown_l
    return residual, None


def reference(hidden_in, norms, w_qkv, w_out, b_out, w_up, b_up, w_down, b_down):
    residual, unused = lax.scan(one_layer, hidden_in.astype(jnp.float32), (norms, w_qkv, w_out, b_out, w_up, b_up, w_down, b_down))
    return residual.astype(jnp.bfloat16)
```

```python
import functools
import math

import jax
import jax.numpy as jnp
from jax import lax
from jax.experimental import pallas as pl
from jax.experimental.pallas import tpu as pltpu
from jax.sharding import PartitionSpec as P

LN_EPS = 1e-5
LOG2E = math.log2(math.e)
SWAP_CORE = [(0, 1), (1, 0), (2, 3), (3, 2)]
SWAP_CHIP = [(0, 2), (2, 0), (1, 3), (3, 1)]


def layer_norm(rows, gain, shift):
    row_mean = jnp.mean(rows, axis=-1, keepdims=True)
    centred = rows - row_mean
    row_var = jnp.mean(centred * centred, axis=-1, keepdims=True)
    return (centred * lax.rsqrt(row_var + LN_EPS) * gain + shift).astype(jnp.bfloat16)


def attn_kernel(q_ref, own_ref, peer_ref, out_ref, vext_ref, *, scale):
    n = own_ref.shape[0]
    bq = q_ref.shape[0]

    @pl.when(pl.program_id(0) == 0)
    def _():
        for i, col in enumerate((512, 640, 896)):
            vext_ref[i, :n, :128] = own_ref[:, col:col + 128]
            vext_ref[i, n:, :128] = peer_ref[:, col:col + 128]
            vext_ref[i, :, 128:] = jnp.ones((2 * n, 128), jnp.bfloat16)

    low = lax.broadcasted_iota(jnp.int32, (bq, 128), 1) < 64
    nt = (((1,), (1,)), ((), ()))
    outs = []
    for head in range(5):
        pair, odd = head // 2, head % 2
        if head < 4:
            q = q_ref[:, pair * 128:(pair + 1) * 128]
            q = jnp.where(low, jnp.zeros_like(q), q) if odd else jnp.where(low, q, jnp.zeros_like(q))
            kcol = 256 + pair * 128
        else:
            q = q_ref[:, 768:896]
            q = jnp.concatenate([jnp.zeros_like(q[:, :64]), q[:, :64]], axis=1)
            kcol = 768
        s_own = lax.dot_general(q, own_ref[:, kcol:kcol + 128], nt, preferred_element_type=jnp.float32)
        s_peer = lax.dot_general(q, peer_ref[:, kcol:kcol + 128], nt, preferred_element_type=jnp.float32)
        top = jnp.maximum(jnp.max(s_own, axis=1, keepdims=True), jnp.max(s_peer, axis=1, keepdims=True))
        p_own = jnp.exp2((s_own - top) * scale).astype(jnp.bfloat16)
        p_peer = jnp.exp2((s_peer - top) * scale).astype(jnp.bfloat16)
        o = jnp.dot(p_own, vext_ref[pair, :n, :], preferred_element_type=jnp.float32)
        o = o + jnp.dot(p_peer, vext_ref[pair, n:, :], preferred_element_type=jnp.float32)
        outs.append(o[:, :128] / o[:, 128:])
    out_ref[:, 0:128] = jnp.where(low, outs[0], outs[1]).astype(jnp.bfloat16)
    out_ref[:, 128:256] = jnp.where(low, outs[2], outs[3]).astype(jnp.bfloat16)
    out_ref[:, 256:320] = outs[4][:, :64].astype(jnp.bfloat16)


def attention(own, peer, block=512):
    n = own.shape[0]
    return pl.pallas_call(
        functools.partial(attn_kernel, scale=64 ** -0.5 * LOG2E),
        grid=(n // block,),
        in_specs=[
            pl.BlockSpec((block, 1024), lambda i: (i, 0)),
            pl.BlockSpec((n, 1024), lambda i: (0, 0)),
            pl.BlockSpec((n, 1024), lambda i: (0, 0)),
        ],
        out_specs=pl.BlockSpec((block, 320), lambda i: (i, 0)),
        out_shape=jax.ShapeDtypeStruct((n, 320), jnp.bfloat16),
        scratch_shapes=[pltpu.VMEM((3, 2 * n, 256), jnp.bfloat16)],
        compiler_params=pltpu.CompilerParams(vmem_limit_bytes=48 * 2 ** 20),
        cost_estimate=pl.CostEstimate(flops=5 * 4 * n * 2 * n * 256, bytes_accessed=6 * 2 ** 20, transcendentals=10 * n * n),
    )(own, own, peer)


def solution(mesh):
    def swap_core(a):
        return lax.ppermute(a, 'tp', SWAP_CORE)

    def swap_chip(a):
        return lax.ppermute(a, 'tp', SWAP_CHIP)

    def local_layers(hidden_in, norms, w_qkv, w_out, b_out, w_up, b_up, w_down, b_down):
        n_layers = w_qkv.shape[0]
        model = w_qkv.shape[1]
        chip = lax.axis_index('tp') // 2
        group = lax.axis_index('dp')
        n_groups = mesh.shape['dp']

        def far_of(a):
            rows = a.shape[0] // n_groups
            piece = lax.dynamic_slice_in_dim(a, group * rows, rows, 0)
            return lax.all_gather(swap_chip(piece), 'dp', axis=0, tiled=True)

        def four(own, gather=True):
            far = far_of(own) if gather else swap_chip(own)
            return [own, swap_core(own), far, swap_core(far)]

        kept = lax.dynamic_index_in_dim(hidden_in, chip, 0, keepdims=False)
        visiting = swap_chip(lax.dynamic_index_in_dim(hidden_in, 1 - chip, 0, keepdims=False))
        block = kept.shape[0]
        residual = jnp.concatenate([kept, visiting], axis=0).astype(jnp.float32)

        for l in range(n_layers):
            wt = jnp.transpose(w_qkv[l], (1, 2, 3, 0))
            wt = jnp.concatenate([wt[0, :4], wt[1, :4], wt[2, :4], wt[:, 4], jnp.zeros_like(wt[0, :1])], axis=0).reshape(1024, model)
            qkv_sh = four(wt)
            out_sh = four(w_out[l].reshape(-1, model), gather=False)
            up_sh = four(w_up[l])
            down_sh = four(w_down[l])
            bup_sh = four(b_up[l], gather=False)

            normed = layer_norm(residual, norms[l, 0], norms[l, 1])
            total = residual + b_out[l]
            qkv = [lax.dot_general(normed, w, (((1,), (1,)), ((), ())), preferred_element_type=jnp.float32).astype(jnp.bfloat16) for w in qkv_sh]
            for s in range(4):
                attn = attention(qkv[s], swap_core(qkv[s ^ 1]))
                total = total + jnp.dot(attn, out_sh[s], preferred_element_type=jnp.float32)
            residual = total

            def mlp(rows):
                normed2 = layer_norm(rows, norms[l, 2], norms[l, 3])
                acc = rows + b_down[l]
                for s in range(4):
                    u = jnp.dot(normed2, up_sh[s], preferred_element_type=jnp.float32) + bup_sh[s]
                    u = jax.nn.gelu(u, approximate=True).astype(jnp.bfloat16)
                    acc = acc + jnp.dot(u, down_sh[s], preferred_element_type=jnp.float32)
                return acc

            if l < n_layers - 1:
                residual = mlp(residual)
            else:
                back = swap_chip(mlp(residual[block:]).astype(jnp.bfloat16))
                stay = mlp(residual[:block]).astype(jnp.bfloat16)
        first = chip == 0
        return jnp.stack([jnp.where(first, stay, back), jnp.where(first, back, stay)])

    in_specs = (P('dp', 'tp', None), P(), P(None, None, None, 'tp', None), P(None, 'tp', None, None), P(), P(None, None, 'tp'), P(None, 'tp'), P(None, 'tp', None), P())
    return jax.shard_map(local_layers, mesh=mesh, in_specs=in_specs, out_specs=P('dp', 'tp', None), check_vma=False)
```

```python
import functools
import math

import jax
import jax.numpy as jnp
from jax import lax
from jax.experimental import pallas as pl
from jax.experimental.pallas import tpu as pltpu
from jax.sharding import PartitionSpec as P

LN_EPS = 1e-5
LOG2E = math.log2(math.e)
SWAP_CORE = [(0, 1), (1, 0), (2, 3), (3, 2)]
SWAP_CHIP = [(0, 2), (2, 0), (1, 3), (3, 1)]


def layer_norm(rows, gain, shift):
    row_mean = jnp.mean(rows, axis=-1, keepdims=True)
    centred = rows - row_mean
    row_var = jnp.mean(centred * centred, axis=-1, keepdims=True)
    return (centred * lax.rsqrt(row_var + LN_EPS) * gain + shift).astype(jnp.bfloat16)


def attn_kernel(q_ref, own_ref, peer_ref, out_ref, vext_ref, *, scale):
    n = own_ref.shape[0]
    bq = q_ref.shape[0]

    @pl.when(pl.program_id(0) == 0)
    def _():
        vext_ref[:, :, 128:] = jnp.ones((3, 2 * n, 128), jnp.bfloat16)
        for i, col in enumerate((640, 768, 896)):
            vext_ref[i, :n, :128] = own_ref[:, col:col + 128]
            vext_ref[i, n:, :128] = peer_ref[:, col:col + 128]

    low = lax.broadcasted_iota(jnp.int32, (bq, 128), 1) < 64
    nt = (((1,), (1,)), ((), ()))
    outs = []
    for head in range(5):
        q = q_ref[:, head // 2 * 128:(head // 2 + 1) * 128]
        q = jnp.concatenate([q[:, 64:], q[:, :64]], axis=1)
        q = jnp.where(low, jnp.zeros_like(q), q) if head % 2 == 0 else jnp.where(low, q, jnp.zeros_like(q))
        kcol = (head + 5) // 2 * 128
        pair = head // 2
        s_own = lax.dot_general(q, own_ref[:, kcol:kcol + 128], nt, preferred_element_type=jnp.float32)
        s_peer = lax.dot_general(q, peer_ref[:, kcol:kcol + 128], nt, preferred_element_type=jnp.float32)
        top = jnp.maximum(jnp.max(s_own, axis=1, keepdims=True), jnp.max(s_peer, axis=1, keepdims=True))
        p_own = jnp.exp2((s_own - top) * scale).astype(jnp.bfloat16)
        p_peer = jnp.exp2((s_peer - top) * scale).astype(jnp.bfloat16)
        o = jnp.dot(p_own, vext_ref[pair, :n, :], preferred_element_type=jnp.float32)
        o = o + jnp.dot(p_peer, vext_ref[pair, n:, :], preferred_element_type=jnp.float32)
        outs.append(o[:, :128] / o[:, 128:])
    out_ref[:, 0:128] = jnp.where(low, outs[0], outs[1]).astype(jnp.bfloat16)
    out_ref[:, 128:256] = jnp.where(low, outs[2], outs[3]).astype(jnp.bfloat16)
    out_ref[:, 256:320] = outs[4][:, :64].astype(jnp.bfloat16)


def whole(a):
    return pl.BlockSpec(a.shape, lambda i: (0,) * a.ndim)


def row_block(block, width):
    return pl.BlockSpec((block, width), lambda i: (i, 0))


def of_layer(w, layer):
    index = layer if w.shape[0] > 1 else 0
    return pl.BlockSpec((1,) + w.shape[1:], lambda i: (index, 0, 0))


def qkv_kernel(h_ref, w0_ref, w1_ref, out0_ref, out1_ref):
    f = w0_ref.shape[1]
    for w, out in ((w0_ref, out0_ref), (w1_ref, out1_ref)):
        out[:, f:] = jnp.zeros((out.shape[0], out.shape[1] - f), jnp.bfloat16)
        out[:, :f] = lax.dot_general(h_ref[...], w[0], (((1,), (1,)), ((), ())), preferred_element_type=jnp.float32).astype(jnp.bfloat16)


def project(h, w0, w1, layer, block=256):
    n, d = h.shape
    f = w0.shape[1]
    return pl.pallas_call(
        qkv_kernel,
        grid=(n // block,),
        in_specs=[row_block(block, d), of_layer(w0, layer), of_layer(w1, layer)],
        out_specs=(row_block(block, 1024),) * 2,
        out_shape=(jax.ShapeDtypeStruct((n, 1024), jnp.bfloat16),) * 2,
        compiler_params=pltpu.CompilerParams(vmem_limit_bytes=40 * 2 ** 20),
        cost_estimate=pl.CostEstimate(flops=4 * n * d * f, bytes_accessed=2 * n * d + 4 * f * d + 4 * n * f, transcendentals=0),
    )(h, w0, w1)


def out_kernel(r_ref, bias_ref, norm_ref, a0, a1, a2, a3, w0, w1, w2, w3, r_out, h_out):
    acc = r_ref[...] + bias_ref[...]
    for a, w in ((a0, w0), (a1, w1), (a2, w2), (a3, w3)):
        acc = acc + jnp.dot(a[...], w[0], preferred_element_type=jnp.float32)
    r_out[...] = acc
    h_out[...] = layer_norm(acc, norm_ref[0:1, :], norm_ref[1:2, :])


def out_proj(r, bias, norm, attns, ws, layer, block=256):
    n, d = r.shape
    f = attns[0].shape[1]
    return pl.pallas_call(
        out_kernel,
        grid=(n // block,),
        in_specs=[row_block(block, d), whole(bias), whole(norm)] + [row_block(block, f)] * 4 + [of_layer(w, layer) for w in ws],
        out_specs=(row_block(block, d),) * 2,
        out_shape=(jax.ShapeDtypeStruct((n, d), jnp.float32), jax.ShapeDtypeStruct((n, d), jnp.bfloat16)),
        compiler_params=pltpu.CompilerParams(vmem_limit_bytes=40 * 2 ** 20),
        cost_estimate=pl.CostEstimate(flops=8 * n * d * f, bytes_accessed=12 * n * d + 8 * f * d, transcendentals=0),
    )(r, bias, norm, *attns, *ws)


def mlp_kernel(h_ref, r_ref, bdown_ref, bias_ref, norm_ref, *refs, pick, normed):
    count = len(pick)
    ws, refs = refs[:2 * count], refs[2 * count:]
    out_ref, hn_ref = refs[0], refs[1] if normed else None
    up_ref, down_ref, u_ref, acc_ref, sems = refs[1 + normed:]
    first = pl.program_id(0) == 0
    d, f = h_ref.shape[1], u_ref.shape[1]
    chunk = 256

    def copies(s):
        for which, dst in ((0, up_ref), (1, down_ref)):
            yield pltpu.make_async_copy(ws[2 * s + which].at[pick[s][which]], dst.at[s], sems.at[s, which])

    @pl.when(first)
    def _():
        for s in range(count):
            for copy in copies(s):
                copy.start()

    acc_ref[...] = r_ref[...] + bdown_ref[...]
    for s in range(count):
        @pl.when(first)
        def _():
            for copy in copies(s):
                copy.wait()

        for n in range(f // chunk):
            cols = slice(n * chunk, (n + 1) * chunk)
            u = jnp.dot(h_ref[...], up_ref[s, :, :, cols].reshape(d, chunk), preferred_element_type=jnp.float32) + bias_ref[s:s + 1, cols]
            u_ref[:, cols] = jax.nn.gelu(u, approximate=True).astype(jnp.bfloat16)
        for n in range(d // chunk):
            cols = slice(n * chunk, (n + 1) * chunk)
            acc_ref[:, cols] += jnp.dot(u_ref[...], down_ref[s, :, :, cols].reshape(f, chunk), preferred_element_type=jnp.float32)
    out_ref[...] = acc_ref[...].astype(out_ref.dtype)
    if normed:
        hn_ref[...] = layer_norm(acc_ref[...], norm_ref[0:1, :], norm_ref[1:2, :])


def mlp(h, r, bdown, norm, shards, normed=False, dtype=jnp.float32, part=None, block=512):
    d = h.shape[1]
    start, n = part or (0, h.shape[0])
    offset = start // block
    count = len(shards)
    pick = [s[2] for s in shards]
    weights = [w for s in shards for w in s[1]]
    bias = jnp.stack([s[0] for s in shards])
    f = bias.shape[1]
    rows_in = pl.BlockSpec((block, d), lambda i: (i + offset, 0))
    out_shape = [jax.ShapeDtypeStruct((n, d), dtype)]
    if normed:
        out_shape.append(jax.ShapeDtypeStruct((n, d), jnp.bfloat16))
    return pl.pallas_call(
        functools.partial(mlp_kernel, pick=pick, normed=normed),
        grid=(n // block,),
        in_specs=[rows_in, rows_in, whole(bdown), whole(bias), whole(norm)] + [pl.BlockSpec(memory_space=pl.ANY)] * (2 * count),
        out_specs=[row_block(block, d)] * len(out_shape),
        out_shape=out_shape,
        scratch_shapes=[
            pltpu.VMEM((count, 4, d // 4, f), jnp.bfloat16),
            pltpu.VMEM((count, 4, f // 4, d), jnp.bfloat16),
            pltpu.VMEM((block, f), jnp.bfloat16),
            pltpu.VMEM((block, d), jnp.float32),
            pltpu.SemaphoreType.DMA((count, 2)),
        ],
        compiler_params=pltpu.CompilerParams(vmem_limit_bytes=60 * 2 ** 20),
        cost_estimate=pl.CostEstimate(flops=count * 4 * n * d * f, bytes_accessed=count * 4 * d * f + 8 * n * d, transcendentals=count * n * f),
    )(h, r, bdown, bias, norm, *weights)


def attention(own, peer, block=512):
    n = own.shape[0]
    return pl.pallas_call(
        functools.partial(attn_kernel, scale=64 ** -0.5 * LOG2E),
        grid=(n // block,),
        in_specs=[
            row_block(block, 1024),
            whole(own),
            whole(own),
        ],
        out_specs=row_block(block, 320),
        out_shape=jax.ShapeDtypeStruct((n, 320), jnp.bfloat16),
        scratch_shapes=[pltpu.VMEM((3, 2 * n, 256), jnp.bfloat16)],
        compiler_params=pltpu.CompilerParams(vmem_limit_bytes=48 * 2 ** 20),
        cost_estimate=pl.CostEstimate(flops=5 * 4 * n * 2 * n * 256, bytes_accessed=6 * 2 ** 20, transcendentals=10 * n * n),
    )(own, own, peer)


def solution(mesh):
    def swap_core(a):
        return lax.ppermute(a, 'tp', SWAP_CORE)

    def swap_chip(a):
        return lax.ppermute(a, 'tp', SWAP_CHIP)

    def after(a, *earlier):
        return lax.optimization_barrier((a, *earlier))[0]

    def local_layers(hidden_in, norms, w_qkv, w_out, b_out, w_up, b_up, w_down, b_down):
        n_layers, model = w_qkv.shape[:2]
        hidden = w_up.shape[2]
        chip = lax.axis_index('tp') // 2
        group = lax.axis_index('dp')
        n_groups = mesh.shape['dp']

        def piece(a, l):
            rows = a.shape[1] // n_groups
            return lax.dynamic_slice(a, (l, group * rows, 0), (1, rows, a.shape[2]))

        def gathered(a):
            return lax.all_gather(a, 'dp', axis=0, tiled=True)

        sent = lax.dynamic_index_in_dim(hidden_in, 1 - chip, 0, keepdims=False)
        visiting = swap_chip(sent)
        kept = lax.dynamic_index_in_dim(hidden_in, chip, 0, keepdims=False)
        block = kept.shape[0]

        wt = jnp.transpose(w_qkv, (0, 2, 3, 4, 1)).reshape(n_layers, -1, model)
        wo = w_out.reshape(n_layers, -1, model)
        up4 = w_up.reshape(n_layers, 4, model // 4, hidden)
        down4 = w_down.reshape(n_layers, 4, hidden // 4, model)

        def fetch_qkv(l, *earlier):
            return gathered(swap_chip(after(piece(wt, l)[0], *earlier)))[None]

        def fetch_mlp(l, *earlier):
            both = jnp.concatenate([piece(w_up, l), piece(w_down, l)], axis=0)
            return gathered(swap_chip(after(both, *earlier))[None])

        wt_partner = swap_core(after(wt, sent))
        qkv_far = fetch_qkv(0, sent)
        mlp_far = fetch_mlp(0, visiting)
        residual = jnp.concatenate([kept, visiting], axis=0).astype(jnp.float32)
        normed = layer_norm(residual, norms[0, 0], norms[0, 1])

        for l in range(n_layers):
            own, partner = project(normed, wt, wt_partner, l)
            if l == 0:
                wo_partner, up_partner, down_partner, bup_partner = (swap_core(after(a, own)) for a in (wo, up4, down4, b_up))
                bup_far = swap_chip(after(b_up, own))
                bup_diag = swap_core(bup_far)
            attn0 = attention(own, swap_core(partner))
            attn1 = attention(after(partner, attn0), swap_core(own))
            qkv_far = after(qkv_far, attn0)
            out_far = swap_chip(after(wo[l:l + 1], attn0))
            out_diag = swap_core(out_far)
            far, diag = project(after(normed, attn1), qkv_far, swap_core(qkv_far), l)
            attn2 = attention(far, swap_core(diag))
            attn3 = attention(after(diag, attn2), swap_core(far))
            if l + 1 < n_layers:
                qkv_far = fetch_qkv(l + 1, attn3)
            residual, normed2 = out_proj(residual, b_out[l:l + 1], norms[l, 2:4], (attn0, attn1, attn2, attn3), (wo, wo_partner, out_far, out_diag), l)

            mlp_diag = swap_core(mlp_far)
            near = [(b_up[l], (up4, down4), (l, l)), (bup_partner[l], (up_partner, down_partner), (l, l))]
            every = slice(None)
            far_sh = (bup_far[l], (mlp_far, mlp_far), ((every, 0), (every, 1)))
            diag_sh = (bup_diag[l], (mlp_diag, mlp_diag), ((every, 0), (every, 1)))
            bd = b_down[l:l + 1]
            if l + 1 < n_layers:
                norm = norms[l + 1, 0:2]
                residual, = mlp(normed2, residual, bd, norm, near)
                residual, = mlp(normed2, residual, jnp.zeros_like(bd), norm, [far_sh])
                mlp_far = fetch_mlp(l + 1, residual)
                residual, normed = mlp(normed2, residual, jnp.zeros_like(bd), norm, [diag_sh], normed=True)
            else:
                shards = near + [far_sh, diag_sh]
                last, = mlp(normed2, residual, bd, norms[l, 0:2], shards, dtype=jnp.bfloat16, part=(block, block))
                back = swap_chip(last)
                stay, = mlp(after(normed2, last), residual, bd, norms[l, 0:2], shards, dtype=jnp.bfloat16, part=(0, block))
        first = chip == 0
        return jnp.stack([jnp.where(first, stay, back), jnp.where(first, back, stay)])

    in_specs = (P('dp', 'tp', None), P(), P(None, None, None, 'tp', None), P(None, 'tp', None, None), P(), P(None, None, 'tp'), P(None, 'tp'), P(None, 'tp', None), P())
    return jax.shard_map(local_layers, mesh=mesh, in_specs=in_specs, out_specs=P('dp', 'tp', None), check_vma=False)
```
